128 devices in a mesh: row: 16 (over y, z_hi, core), col: 8 (over z_lo, x).
Axes of the slice: x: 4, y: 4, z: 4 (z_hi: 2, z_lo: 2; z = z_hi * 2 + z_lo), core: 2. Of those that a mesh axis runs over, the one named last changes fastest.
Arguments:
- vectors: float32 [32768, 8192], P('row', 'col'), may hold values from -6 to 6
- reflectors: float32 [8, 32768, 128], P('col', 'row'), may hold values from -0.03125 to 0.03125
- triangles: float32 [8, 128, 128], P('col'), may hold values from -0.25 to 1.8, as said below
Outputs:
- transformed: float32 [32768, 8192], P('row', 'col')
The draws below stay inside these ranges and needn't reach their ends.
Inputs may be any that keep to these rules, and one draw needn't show every extreme that they name: Each triangles[p] is upper triangular with diagonal entries between 0.5 and 1.8.
All inputs are finite; a program needn't handle non-finite values.
Results may differ from the reference program's by a relative error of at most 0.00013.
Values sent between devices are 32-bit elements; how exact they have to be, the bound alone decides.
No kernel may reach another device: no remote copies, remote signals or barrier semaphores. Data moves between devices by JAX's collectives and lax.ppermute only.
A program may use at most 128 MiB of HBM per device.

```python
import jax
import jax.numpy as jnp
from jax import lax

ORDER = 32768
NB = 128
PANELS = 8
COLS = 8192


def draw_triangles(key, part):
    first, second = jax.random.split(jax.random.fold_in(key, 7))
    diagonal = jax.random.uniform(first, (PANELS, NB), jnp.float32, 0.5, 1.5)
    offdiag = jnp.clip(0.05 * jax.random.normal(second, (PANELS, NB, NB), jnp.float32), -0.25, 0.25)
    ident = jnp.eye(NB, dtype=jnp.float32)
    return jnp.triu(offdiag, 1) + diagonal[:, :, None] * ident[None, :, :]


def level_of(rng, shape, cuts, low, largest):
    def one(axis_at, shards_of):
        steps = jax.random.uniform(jax.random.fold_in(jax.random.fold_in(rng, 6), axis_at), (shards_of,), jnp.float32, low / len(cuts), largest / len(cuts))
        return jnp.repeat(jnp.exp(steps), shape[axis_at] // shards_of).reshape((-1,) + (1,) * (len(shape) - axis_at - 1))

    gain = one(*cuts[0])
    for cut in cuts[1:]:
        gain = gain * one(*cut)
    return gain


def noise(own_key, extent, scale, bound, shards=(), kind=jnp.bfloat16):
    result = scale * jax.random.normal(own_key, extent, jnp.float32)
    if shards:
        result = result * level_of(own_key, extent, shards, -0.22, 0.18)
    return jnp.clip(result, -bound, bound).astype(kind)


def setup_inputs(seed: int = 0) -> dict:
    key_list = jax.random.split(jax.random.key(seed), 4)
    vectors = noise(key_list[0], (ORDER, COLS), 1.0, 6.0, ((0, 16), (1, 8)), jnp.float32)
    reflectors = noise(key_list[1], (PANELS, ORDER, NB), ORDER ** -0.5, 0.03125, ((0, 8), (1, 16)), jnp.float32)
    triangles = draw_triangles(jax.random.fold_in(key_list[3], 71), 0)
    return dict(vectors=vectors, reflectors=reflectors, triangles=triangles)


def reference(vectors, reflectors, triangles):
    hi = lax.Precision.HIGHEST
    block = vectors
    for panel in range(PANELS - 1, -1, -1):
        basis = reflectors[panel]
        summed = lax.dot_general(basis, block, (((0,), (0,)), ((), ())), precision=hi, preferred_element_type=jnp.float32)
        scaled = jnp.dot(triangles[panel], summed, precision=hi, preferred_element_type=jnp.float32)
        block = block - jnp.dot(basis, scaled, precision=hi, preferred_element_type=jnp.float32)
    return block
```

```python
import jax
import jax.numpy as jnp
from jax import lax
from jax.experimental import pallas as pl
from jax.experimental.pallas import tpu as pltpu
from jax.sharding import Mesh
from jax.sharding import PartitionSpec as P

ROW = ("y", "zh", "k")
COL = ("zl", "x")
STEP = 512
F32 = jnp.float32
BF16 = jnp.bfloat16


def shifted(value, axis, by):
    peers = lax.axis_size(axis)
    return lax.ppermute(value, axis, [(i, (i + by) % peers) for i in range(peers)])


def halves(value):
    high = value.astype(BF16)
    return high, (value - high.astype(F32)).astype(BF16)


def dot(left, right, dims):
    return lax.dot_general(left, right, (dims, ((), ())), preferred_element_type=F32)


def dot_split(left, right, dims):
    (lh, ll), (rh, rl) = left, right
    (a,), (b,) = dims
    return dot(jnp.concatenate([lh, ll, lh], axis=a), jnp.concatenate([rh, rh, rl], axis=b), dims)


ROWS = ((0,), (0,))
PLAIN = ((1,), (0,))


def call(kernel, grid, ins, outs, scratch, operands, aliases=None, flops=0):
    return pl.pallas_call(
        kernel,
        grid_spec=pltpu.PrefetchScalarGridSpec(
            num_scalar_prefetch=1,
            grid=grid,
            in_specs=ins,
            out_specs=[s for s, _ in outs],
            scratch_shapes=scratch,
        ),
        out_shape=[o for _, o in outs],
        input_output_aliases=aliases or {},
        cost_estimate=pl.CostEstimate(flops=flops, bytes_accessed=flops // 256, transcendentals=0),
        compiler_params=pltpu.CompilerParams(
            dimension_semantics=("arbitrary",) * len(grid), vmem_limit_bytes=56 * 1024 * 1024
        ),
    )(*operands)


def shape(*dims, dtype=F32):
    return jax.ShapeDtypeStruct(dims, dtype)


def loaded(refs, panels, i, steps):
    at, rows = 0, []
    for p in panels:
        v = refs[at][...]
        if len(p) == 2:
            v = jnp.where(i < steps // 2, v, refs[at + 1][...])
        at += len(p)
        rows.append(v)
    return rows


def specs_of(panels, steps):
    width, half = panels[0][0].shape[1], steps // 2
    out = []
    for p in panels:
        if len(p) == 1:
            out.append(pl.BlockSpec((STEP, width), lambda i, m: (i, 0)))
        else:
            out.append(pl.BlockSpec((STEP, width), lambda i, m: (jnp.minimum(i, half - 1), 0)))
            out.append(pl.BlockSpec((STEP, width), lambda i, m: (jnp.maximum(i - half, 0), 0)))
    return out


def panel_products(meta, block, panels):
    rows, cols = block.shape
    width = panels[0][0].shape[1]
    total = width * len(panels)
    steps = rows // STEP
    flat = [part for p in panels for part in p]
    piece = cols // 8

    def kernel(m, x_ref, *refs):
        mine, theirs, hi_ref, lo_ref, acc = refs[len(flat) :]
        i = pl.program_id(0)
        whole = loaded(refs, panels, i, steps)
        v = halves(jnp.concatenate(whole, axis=1) if len(whole) > 1 else whole[0])
        hi_ref[...], lo_ref[...] = v
        product = dot_split(v, halves(x_ref[...]), ROWS)

        @pl.when(i == 0)
        def _():
            acc[...] = product

        @pl.when(i > 0)
        def _():
            acc[...] += product

        @pl.when(i == steps - 1)
        def _():
            core, y = m[0], m[1]
            for dy in range(4):
                base = lax.rem(y + dy, 4) * (2 * piece)
                mine[dy] = acc[:, pl.ds(pl.multiple_of(base + core * piece, piece), piece)]
                theirs[dy] = acc[:, pl.ds(pl.multiple_of(base + (1 - core) * piece, piece), piece)]

    ins = [pl.BlockSpec((STEP, cols), lambda i, m: (i, 0)), *specs_of(panels, steps)]
    pieces = (pl.BlockSpec((4, total, piece), lambda i, m: (0, 0, 0)), shape(4, total, piece))
    split = (pl.BlockSpec((STEP, total), lambda i, m: (i, 0)), shape(rows, total, dtype=BF16))
    return call(
        kernel, (steps,), ins, [pieces, pieces, split, split],
        [pltpu.VMEM((total, cols), F32)], (meta, block, *flat), flops=6 * rows * total * cols,
    )


def inner_products(meta, panels, tri, share):
    rows, width = panels[0][0].shape
    steps = rows // STEP
    part = width // 4
    flat = [p for panel in panels for p in panel]

    def kernel(m, *refs):
        tri_ref, out, left_own, own_both, across_both = refs[len(flat) :]
        i = pl.program_id(0)
        own, left, across, far = loaded(refs, panels, i, steps)

        @pl.when(i == 0)
        def _():
            for acc in (left_own, own_both, across_both):
                acc[...] = jnp.zeros_like(acc)

        own, left, across, far = halves(own), halves(left), halves(across), halves(far)

        def beside(a, b):
            return tuple(jnp.concatenate([u, v], axis=1) for u, v in zip(a, b))

        left_own[...] += dot_split(left, own, ROWS)
        own_both[...] += dot_split(own, beside(far, across), ROWS)
        across_both[...] += dot_split(across, beside(left, far), ROWS)

        @pl.when(i == steps - 1)
        def _():
            for y in range(4):
                r = slice(y * part, (y + 1) * part)
                out[y, 0, 0] = left_own[r]
                out[y, 0, 1] = own_both[r, :width]
                out[y, 0, 2] = own_both[r, width:]
                out[y, 1, 0] = across_both[r, :width]
                out[y, 1, 1] = across_both[r, width:]
                out[y, 1, 2] = tri_ref[r] * share

    ins = [*specs_of(panels, steps), pl.BlockSpec((width, width), lambda i, m: (0, 0))]
    dims = (4, 2, 3, part, width)
    return call(
        kernel, (steps,), ins, [(pl.BlockSpec(dims, lambda i, m: (0,) * 5), shape(*dims))],
        [pltpu.VMEM((width, width), F32)] + [pltpu.VMEM((width, 2 * width), F32)] * 2,
        (meta, *flat, tri), flops=30 * rows * width * width,
    )[0]


def coupling(meta, kept, other):
    width = kept.shape[-1]

    def kernel(m, a_ref, b_ref, g_ref, t_ref):
        def fill(low, high):
            def block(b, c):
                ref, b = (low, b) if b < 3 else (high, b - 3)
                return jnp.concatenate([ref[y, c, b] for y in range(4)], axis=0)

            def put(p, q, value):
                g_ref[p, :, pl.ds(q * width, width)] = value

            for c in range(8):
                z, x = divmod(c, 4)
                left, far, across = z * 4 + (x + 3) % 4, z * 4 + (x + 2) % 4, (1 - z) * 4 + x
                for p, q, b in ((left, c, 0), (c, far, 1), (c, across, 2), (across, left, 3), (across, far, 4)):
                    if p < q:
                        put(p, q, block(b, c))
                    elif b in (0, 3):
                        put(q, p, block(b, c).T)
                t_ref[c] = block(5, c)

        @pl.when(m[0] == 0)
        def _():
            fill(a_ref, b_ref)

        @pl.when(m[0] != 0)
        def _():
            fill(b_ref, a_ref)

    every = pl.BlockSpec(kept.shape, lambda i, m: (0,) * 5)
    outs = [
        (pl.BlockSpec((8, width, 8 * width), lambda i, m: (0, 0, 0)), shape(8, width, 8 * width)),
        (pl.BlockSpec((8, width, width), lambda i, m: (0, 0, 0)), shape(8, width, width)),
    ]
    return call(kernel, (1,), [every, every], outs, [], (meta, kept, other))


def solved(meta, sums, inner, tri):
    width = tri.shape[-1]
    cols = sums[0].shape[1]

    def kernel(m, *refs):
        parts, (g_ref, t_ref, out, w, y) = refs[: len(sums)], refs[len(sums) :]
        at = 0
        for part in parts:
            w[pl.ds(at, part.shape[0]), :] = part[...]
            at += part.shape[0]
        for p in range(7, -1, -1):
            place = pl.ds(pl.multiple_of(m[2 + p] * width, width), width)
            rest = w[place, :]
            if p < 7:
                below = (p + 1) * width
                rest = rest - dot_split(
                    halves(g_ref[p, :, below:]), halves(y[below:, :]), PLAIN
                )
            value = dot_split(halves(t_ref[p]), halves(rest), PLAIN)
            y[pl.ds(p * width, width), :] = value
            out[place, :] = value

    def whole(a):
        return pl.BlockSpec(a.shape, lambda i, m: (0,) * a.ndim)

    spec = pl.BlockSpec((8 * width, cols), lambda i, m: (0, 0))
    return call(
        kernel, (1,), [whole(a) for a in (*sums, inner, tri)], [(spec, shape(8 * width, cols))],
        [pltpu.VMEM((8 * width, cols), F32)] * 2, (meta, *sums, inner, tri), flops=8 * 8 * width * width * width * 6,
    )[0]


def updated(meta, block, bases, ys, offsets, before):
    rows, cols = block.shape
    piece = cols // 8
    order = ys[0][0].shape[0]
    flat_v = [part for b in bases for part in b]
    flat_y = [part for y in ys for part in y]

    def kernel(m, x_ref, *refs):
        n = len(flat_v)
        v_refs, y_refs, (out, hi, lo) = refs[:n], refs[n : n + len(flat_y)], refs[-3:]
        i, j = pl.program_id(0), pl.program_id(1)

        @pl.when((i == 0) & (j == 0))
        def _():
            core = m[0]
            for at in range(len(ys)):
                for half, ref in enumerate(y_refs[2 * at : 2 * at + 2]):
                    place = pl.ds(pl.multiple_of(jnp.where(half == 0, core, 1 - core) * piece, piece), piece)
                    high, low = halves(ref[...])
                    hi[at, :, place] = high
                    lo[at, :, place] = low

        high = [v_refs[2 * b][...] for b in range(len(bases))]
        low = [v_refs[2 * b + 1][...] for b in range(len(bases))]
        v = jnp.concatenate(high + low + high, axis=1)
        out[...] = x_ref[...] - dot(v, jnp.concatenate([hi[j], hi[j], lo[j]], axis=0), PLAIN)

    def where(i, j, m):
        off = jnp.int32(offsets[0])
        for at, o in enumerate(offsets[1:], 1):
            off = jnp.where(j == at, o, off)
        return i, lax.rem(m[1] + off, 4)

    ins = [pl.BlockSpec((STEP, 2 * piece), where)]
    ins += [pl.BlockSpec((STEP, v.shape[1]), lambda i, j, m: (i, 0)) for v in flat_v]
    ins += [pl.BlockSpec((order, piece), lambda i, j, m: (0, 0)) for _ in flat_y]
    operands, aliases = [meta, block, *flat_v, *flat_y], {}
    if before is not None:
        aliases = {len(operands): 0}
        ins.append(pl.BlockSpec(memory_space=pl.ANY))
        operands.append(before)
    scratch = [pltpu.VMEM((len(ys), order, 2 * piece), BF16)] * 2
    return call(
        kernel, (rows // STEP, len(ys)), ins, [(pl.BlockSpec((STEP, 2 * piece), where), shape(rows, cols))],
        scratch, operands, aliases, flops=6 * rows * order * 2 * piece * len(ys),
    )[0]


def near_sum(mine, theirs):
    both = mine + shifted(theirs, "k", 1)
    near = shifted(both[1], "y", 1), shifted(both[3], "y", -1), shifted(both[2], "y", 2)
    return both[0] + near[0] + near[1] + near[2]


def doubled(total):
    return total + shifted(total, "zh", 1)


def from_everyone(piece, axes):
    peers = lax.axis_size(axes)
    return lax.all_to_all(jnp.broadcast_to(piece[None], (peers, *piece.shape)), axes, 0, 0, tiled=True)


def shards(vectors, reflectors, triangles):
    own, tri = reflectors[0], triangles[0]
    core, y, z, x = (lax.axis_index(a) for a in ("k", "y", "zl", "x"))
    places = []
    for p in range(8):
        pz, px = divmod(p, 4)
        dx = lax.rem(px - x + 4, 4)
        same = jnp.where(dx == 0, 0, jnp.where(dx == 3, 1, jnp.where(dx == 1, 2, 4)))
        cross = jnp.where(dx == 0, 3, jnp.where(dx == 3, 5, jnp.where(dx == 1, 6, 7)))
        places.append(jnp.where(pz == z, same, cross))
    meta = jnp.stack([core, y, *places]).astype(jnp.int32)
    return body(meta, vectors, own, tri)


def body(meta, vectors, own, tri):
    half = own.shape[0] // 2
    upper, lower = own[:half], own[half:]
    left0, right1 = shifted(upper, "x", 1), shifted(lower, "x", -1)
    across = shifted(own, "zl", 1)
    left1, right0 = shifted(lower, "x", 1), shifted(upper, "x", -1)
    far = shifted(left0, "x", 1), shifted(right1, "x", -1)
    left, right = (left0, left1), (right0, right1)
    across_left, across_right = shifted(across, "x", 1), shifted(across, "x", -1)
    across_far = shifted(far[0], "zl", 1), shifted(far[1], "zl", 1)

    m0, t0, h0, l0 = panel_products(meta, vectors, [(own,)])
    sum0 = near_sum(m0, t0)
    m1, t1, h1, l1 = panel_products(meta, vectors, [left, right, (across,)])
    ginner = inner_products(meta, [(own,), left, (across,), far], tri, 1.0 / 16.0)
    parts = lax.all_to_all(ginner.reshape(8, *ginner.shape[2:]), ("y", "k"), 0, 0, tiled=True)
    gsum = jnp.sum(parts, axis=0)
    gsum = doubled(gsum)
    sum1 = near_sum(m1, t1)
    early = doubled(jnp.concatenate([sum0, sum1]))
    gall = from_everyone(gsum, ("y", "zl", "x")).reshape(4, 8, *gsum.shape)
    inner, tris = coupling(meta, gall, shifted(gall, "k", 1))
    m2, t2, h2, l2 = panel_products(meta, vectors, [far, (across_left,), (across_right,), across_far])
    late = doubled(near_sum(m2, t2))
    ys = solved(meta, (early, late), inner, tris)

    bases = (h0, l0), (h1, l1), (h2, l2)
    ahead, behind = shifted(ys, "y", -1), shifted(ys, "y", 1)
    out = updated(meta, vectors, bases, [(ys, shifted(ys, "k", 1))], (0,), None)
    top = ys.shape[0] // 2
    away = shifted(ahead[:top], "y", -1), shifted(behind[top:], "y", 1)
    side = [(v, shifted(v, "k", 1)) for v in (ahead, behind)]
    out = updated(meta, vectors, bases, side, (1, 3), out)
    away = jnp.concatenate(away)
    return updated(meta, vectors, bases, [(away, shifted(away, "k", 1))], (2,), out)


def solution(mesh):
    torus = Mesh(mesh.devices.reshape(4, 2, 2, 2, 4), ROW + COL)
    return jax.shard_map(
        shards,
        mesh=torus,
        in_specs=(P(ROW, COL), P(COL, ROW, None), P(COL, None, None)),
        out_specs=P(ROW, COL),
        check_vma=False,
    )
```

```python
import jax
import jax.numpy as jnp
from jax import lax
from jax.experimental import pallas as pl
from jax.experimental.pallas import tpu as pltpu
from jax.sharding import Mesh
from jax.sharding import PartitionSpec as P

ROW = ("y", "zh", "k")
COL = ("zl", "x")
STEP = 512
WIDE = 512
F32 = jnp.float32
BF16 = jnp.bfloat16


def shifted(value, axis, by):
    peers = lax.axis_size(axis)
    return lax.ppermute(value, axis, [(i, (i + by) % peers) for i in range(peers)])


def halves(value):
    high = value.astype(BF16)
    return high, (value - high.astype(F32)).astype(BF16)


def dot(left, right, dims):
    return lax.dot_general(left, right, (dims, ((), ())), preferred_element_type=F32)


def dot_split(left, right, dims):
    (lh, ll), (rh, rl) = left, right
    (a,), (b,) = dims
    return dot(jnp.concatenate([lh, ll, lh], axis=a), jnp.concatenate([rh, rh, rl], axis=b), dims)


ROWS = ((0,), (0,))
PLAIN = ((1,), (0,))


def call(kernel, grid, ins, outs, scratch, operands, aliases=None, flops=0):
    return pl.pallas_call(
        kernel,
        grid_spec=pltpu.PrefetchScalarGridSpec(
            num_scalar_prefetch=1,
            grid=grid,
            in_specs=ins,
            out_specs=[s for s, _ in outs],
            scratch_shapes=scratch,
        ),
        out_shape=[o for _, o in outs],
        input_output_aliases=aliases or {},
        cost_estimate=pl.CostEstimate(flops=flops, bytes_accessed=flops // 256, transcendentals=0),
        compiler_params=pltpu.CompilerParams(
            dimension_semantics=("arbitrary",) * len(grid), vmem_limit_bytes=20 * 1024 * 1024
        ),
    )(*operands)


def onchip(*dims, dtype=F32):
    return pl.BlockSpec(memory_space=pltpu.VMEM), pltpu.VMEM(dims, dtype)


ONCHIP = pl.BlockSpec(memory_space=pltpu.VMEM)


def held(meta, block):
    rows, cols = block.shape

    def kernel(m, x_ref, high, low):
        here = pl.ds(pl.multiple_of(pl.program_id(0) * STEP, STEP), STEP)
        high[here, :], low[here, :] = halves(x_ref[...])

    ins = [pl.BlockSpec((STEP, cols), lambda i, m: (i, 0))]
    return call(kernel, (rows // STEP,), ins, [onchip(rows, cols, dtype=BF16)] * 2, [], (meta, block))


def resident(value):
    return pltpu.with_memory_space_constraint(value, pltpu.VMEM)


def shape(*dims, dtype=F32):
    return jax.ShapeDtypeStruct(dims, dtype)


def loaded(refs, panels, i, steps):
    at, rows = 0, []
    for p in panels:
        v = refs[at][...]
        if len(p) == 2:
            v = jnp.where(i < steps // 2, v, refs[at + 1][...])
        at += len(p)
        rows.append(v)
    return rows


def specs_of(panels, steps):
    width, half = panels[0][0].shape[1], steps // 2
    out = []
    for p in panels:
        if len(p) == 1:
            out.append(pl.BlockSpec((STEP, width), lambda i, m: (i, 0)))
        else:
            out.append(pl.BlockSpec((STEP, width), lambda i, m: (jnp.minimum(i, half - 1), 0)))
            out.append(pl.BlockSpec((STEP, width), lambda i, m: (jnp.maximum(i - half, 0), 0)))
    return out


def panel_products(meta, block, panels):
    rows, cols = block[0].shape
    width = panels[0][0].shape[1]
    total = width * len(panels)
    steps = rows // STEP
    flat = [part for p in panels for part in p]
    piece = cols // 8

    def kernel(m, xh_ref, xl_ref, *refs):
        mine, theirs, hi_ref, lo_ref, acc = refs[len(flat) :]
        i = pl.program_id(0)
        whole = loaded(refs, panels, i, steps)
        v = halves(jnp.concatenate(whole, axis=1) if len(whole) > 1 else whole[0])
        here = pl.ds(pl.multiple_of(i * STEP, STEP), STEP)
        hi_ref[here, :], lo_ref[here, :] = v
        product = dot_split(v, (xh_ref[here, :], xl_ref[here, :]), ROWS)

        @pl.when(i == 0)
        def _():
            acc[...] = product

        @pl.when(i > 0)
        def _():
            acc[...] += product

        @pl.when(i == steps - 1)
        def _():
            core, y = m[0], m[1]
            for dy in range(4):
                base = lax.rem(y + dy, 4) * (2 * piece)
                mine[dy] = acc[:, pl.ds(pl.multiple_of(base + core * piece, piece), piece)]
                theirs[dy] = acc[:, pl.ds(pl.multiple_of(base + (1 - core) * piece, piece), piece)]

    ins = [ONCHIP, ONCHIP, *specs_of(panels, steps)]
    pieces = (pl.BlockSpec((4, total, piece), lambda i, m: (0, 0, 0)), shape(4, total, piece))
    split = onchip(rows, total, dtype=BF16)
    return call(
        kernel, (steps,), ins, [pieces, pieces, split, split],
        [pltpu.VMEM((total, cols), F32)], (meta, *map(resident, block), *flat), flops=6 * rows * total * cols,
    )


def inner_products(meta, panels, kept, sent_on):
    rows, width = panels[0][0].shape
    steps = rows // STEP
    deep = kept.shape[1]
    half = width // 2
    flat = [p for panel in panels for p in panel]

    def kernel(m, *refs):
        kept_ref, sent_ref, mine, theirs, sums = refs[len(flat) :]
        i = pl.program_id(0)
        own, left, across, far = loaded(refs, panels, i, steps)
        firsts = m[2] < 2, m[3] == 0, m[3] != 0

        @pl.when(i == 0)
        def _():
            sums[...] = jnp.zeros_like(sums)
            for dy in range(4):
                mine[dy * deep : (dy + 1) * deep] = kept_ref[dy]
                theirs[dy * deep : (dy + 1) * deep] = sent_ref[dy]

        sums[0] += dot_split(halves(left), halves(own), ROWS)
        sums[1] += dot_split(halves(across), halves(left), ROWS)
        for at, (first, a, b) in enumerate(zip(firsts, (own, own, across), (far, across, far)), 2):
            upper, lower = jnp.where(first, a, b), jnp.where(first, b, a)
            sums[at] += dot_split(halves(upper), halves(lower), ROWS)

        def fill(low, high):
            end = 4 * deep
            starts = [pl.multiple_of(jnp.where(first, 0, half), half) for first in firsts]
            low[end : end + width] = sums[0]
            high[end : end + width] = sums[1]
            low[end + width : end + width + half] = sums[2, pl.ds(starts[0], half), :]
            high[end + width : end + width + half] = sums[4, pl.ds(starts[2], half), :]
            shared = sums[3, pl.ds(starts[1], half), :]
            low[end + width + half :] = shared[: half // 2]
            high[end + width + half :] = shared[half // 2 :]

        @pl.when((i == steps - 1) & (m[0] == 0))
        def _():
            fill(mine, theirs)

        @pl.when((i == steps - 1) & (m[0] != 0))
        def _():
            fill(theirs, mine)

    ins = [*specs_of(panels, steps), ONCHIP, ONCHIP]
    dims = (4 * deep + width + half + half // 2, width)
    out = (pl.BlockSpec(dims, lambda i, m: (0, 0)), shape(*dims))
    return call(
        kernel, (steps,), ins, [out, out], [pltpu.VMEM((5, width, width), F32)],
        (meta, *flat, kept, sent_on), flops=30 * rows * width * width,
    )


def coupling(meta, kept, other):
    width = kept.shape[-1]
    half = width // 2

    def kernel(m, a_ref, b_ref, gh, gl, th, tl):
        def put(p, q, start, value):
            r = slice(p * width + start, p * width + start + value.shape[0])
            gh[q, r], gl[q, r] = halves(value)

        def fill(low, high):
            for c in range(8):
                z, x = divmod(c, 4)
                left, far, across = z * 4 + (x + 3) % 4, z * 4 + (x + 2) % 4, (1 - z) * 4 + x
                for p, q, ref in ((left, c, low), (across, left, high)):
                    value = ref[c, :width]
                    put(min(p, q), max(p, q), 0, value if p < q else value.T)
                for p, q, ref in ((c, far, low), (across, far, high)):
                    start = 0 if p < q else half
                    put(min(p, q), max(p, q), start, ref[c, width : width + half])
                start = 0 if c < across else half
                for at, ref in enumerate((low, high)):
                    begin = width + half
                    value = ref[c, begin : begin + half // 2]
                    put(min(c, across), max(c, across), start + at * (half // 2), value)
                    begin += half // 2
                    r = slice(at * half, (at + 1) * half)
                    th[c, r], tl[c, r] = halves(ref[c, begin : begin + half])

        @pl.when(m[0] == 0)
        def _():
            fill(a_ref, b_ref)

        @pl.when(m[0] != 0)
        def _():
            fill(b_ref, a_ref)

    outs = [onchip(8, 8 * width, width, dtype=BF16)] * 2 + [onchip(8, width, width, dtype=BF16)] * 2
    return call(kernel, (1,), [ONCHIP, ONCHIP], outs, [], (meta, kept, other))


def solved(meta, sums, inner):
    width = inner[2].shape[-1]
    cols = sums[0].shape[1]

    def kernel(m, *refs):
        parts, (gh, gl, th, tl, out, w, rest) = refs[: len(sums)], refs[len(sums) :]
        at = 0
        for part in parts:
            depth = part.shape[0] // width * width
            w[pl.ds(at, depth), :] = part[:depth, :]
            at += depth
        places = [pl.ds(pl.multiple_of(m[4 + p] * width, width), width) for p in range(8)]
        for p in range(8):
            rest[pl.ds(p * width, width), :] = w[places[p], :]
        for p in range(7, -1, -1):
            value = dot_split((th[p], tl[p]), halves(rest[pl.ds(p * width, width), :]), PLAIN)
            out[places[p], :] = value
            if p:
                above = pl.ds(0, p * width)
                rest[above, :] -= dot_split((gh[p, above], gl[p, above]), halves(value), PLAIN)

    spec = pl.BlockSpec((8 * width, cols), lambda i, m: (0, 0))
    return call(
        kernel, (1,), [ONCHIP] * (len(sums) + 4), [(spec, shape(8 * width, cols))],
        [pltpu.VMEM((8 * width, cols), F32)] * 2, (meta, *sums, *map(resident, inner)), flops=8 * 8 * width * width * width * 6,
    )[0]


def updated(meta, block, bases, ys, offsets, before):
    rows, cols = block.shape
    piece = cols // 8
    order = ys[0][0].shape[0]
    flat_v = [part for b in bases for part in b]
    flat_y = [part for y in ys for part in y]

    def kernel(m, x_ref, *refs):
        n = len(flat_v)
        v_refs, y_refs, (out, hi, lo) = refs[:n], refs[n : n + len(flat_y)], refs[-3:]
        i, j = pl.program_id(0), pl.program_id(1)

        @pl.when((i == 0) & (j == 0))
        def _():
            core = m[0]
            for at in range(len(ys)):
                for half, ref in enumerate(y_refs[2 * at : 2 * at + 2]):
                    place = pl.ds(pl.multiple_of(jnp.where(half == 0, core, 1 - core) * piece, piece), piece)
                    high, low = halves(ref[...])
                    hi[at, :, place] = high
                    lo[at, :, place] = low

        here = pl.ds(pl.multiple_of(i * WIDE, WIDE), WIDE)
        high = [v_refs[2 * b][here, :] for b in range(len(bases))]
        low = [v_refs[2 * b + 1][here, :] for b in range(len(bases))]
        v = jnp.concatenate(high + low + high, axis=1)
        out[...] = x_ref[...] - dot(v, jnp.concatenate([hi[j], hi[j], lo[j]], axis=0), PLAIN)

    def where(i, j, m):
        off = jnp.int32(offsets[0])
        for at, o in enumerate(offsets[1:], 1):
            off = jnp.where(j == at, o, off)
        return i, lax.rem(m[1] + off, 4)

    ins = [pl.BlockSpec((WIDE, 2 * piece), where)] + [ONCHIP] * (len(flat_v) + len(flat_y))
    operands, aliases = [meta, block, *map(resident, flat_v), *flat_y], {}
    if before is not None:
        aliases = {len(operands): 0}
        ins.append(pl.BlockSpec(memory_space=pl.ANY))
        operands.append(before)
    scratch = [pltpu.VMEM((len(ys), order, 2 * piece), BF16)] * 2
    return call(
        kernel, (rows // WIDE, len(ys)), ins, [(pl.BlockSpec((WIDE, 2 * piece), where), shape(rows, cols))],
        scratch, operands, aliases, flops=6 * rows * order * 2 * piece * len(ys),
    )[0]


def near_sum(mine, theirs):
    received = shifted(theirs, "k", 1)
    both = [m + r for m, r in zip(mine, received)]
    near = shifted(both[1], "y", 1), shifted(both[3], "y", -1), shifted(both[2], "y", 2)
    return both[0] + near[0] + near[1] + near[2]


def near_sum_behind(mine, theirs, deep):
    both = mine + shifted(theirs, "k", 1)

    def with_rest(at):
        return jnp.concatenate([both[at * deep : (at + 1) * deep], both[4 * deep :]])

    near = shifted(with_rest(1), "y", 1), shifted(both[3 * deep :], "y", -1), shifted(with_rest(2), "y", 2)
    return with_rest(0) + near[0] + near[1] + near[2]


def doubled(total):
    return total + shifted(total, "zh", 1)


def from_everyone(piece, axes):
    peers = lax.axis_size(axes)
    return lax.all_to_all(jnp.broadcast_to(piece[None], (peers, *piece.shape)), axes, 0, 0, tiled=True)


def shards(vectors, reflectors, triangles):
    own, tri = reflectors[0], triangles[0]
    core, y, z, x = (lax.axis_index(a) for a in ("k", "y", "zl", "x"))
    places = []
    for p in range(8):
        pz, px = divmod(p, 4)
        dx = lax.rem(px - x + 4, 4)
        same = jnp.where(dx == 0, 0, jnp.where(dx == 3, 1, jnp.where(dx == 1, 2, 4)))
        cross = jnp.where(dx == 0, 3, jnp.where(dx == 3, 5, jnp.where(dx == 1, 6, 7)))
        places.append(jnp.where(pz == z, same, cross))
    meta = jnp.stack([core, y, x, z, *places]).astype(jnp.int32)
    return body(meta, vectors, own, tri)


def body(meta, vectors, own, tri):
    half = own.shape[0] // 2
    split = held(meta, vectors)
    upper, lower = own[:half], own[half:]
    left0, right1 = shifted(upper, "x", 1), shifted(lower, "x", -1)
    across = shifted(own, "zl", 1)
    left1, right0 = shifted(lower, "x", 1), shifted(upper, "x", -1)
    far = shifted(left0, "x", 1), shifted(right1, "x", -1)
    left, right = (left0, left1), (right0, right1)
    across_left, across_right = shifted(across, "x", 1), shifted(across, "x", -1)
    across_far = shifted(far[0], "zl", 1), shifted(far[1], "zl", 1)

    m0, t0, h0, l0 = panel_products(meta, split, [(own,)])
    sum0 = near_sum(m0, t0)
    m1, t1, h1, l1 = panel_products(meta, split, [left, right, (across,)])
    deep = m1.shape[1]
    m1, t1 = inner_products(meta, [(own,), left, (across,), far], m1, t1)
    sum1 = near_sum_behind(m1, t1, deep)
    gsum = doubled(sum1[deep:])
    early = doubled(jnp.concatenate([sum0, sum1[:deep]]))
    width = tri.shape[0]
    part = lax.dynamic_slice_in_dim(tri, meta[0] * (width // 2), width // 2)
    gall = from_everyone(jnp.concatenate([gsum, part]), ("zl", "x"))
    inner = coupling(meta, gall, shifted(gall, "k", 1))
    m2, t2, h2, l2 = panel_products(meta, split, [far, (across_left,), (across_right,), across_far])
    late = doubled(near_sum(m2, t2))
    ys = solved(meta, (early, late), inner)

    bases = (h0, l0), (h1, l1), (h2, l2)
    ahead, behind = shifted(ys, "y", -1), shifted(ys, "y", 1)
    out = updated(meta, vectors, bases, [(ys, shifted(ys, "k", 1))], (0,), None)
    top = ys.shape[0] // 2
    away = shifted(ahead[:top], "y", -1), shifted(behind[top:], "y", 1)
    side = [(v, shifted(v, "k", 1)) for v in (ahead, behind)]
    out = updated(meta, vectors, bases, side, (1, 3), out)
    away = jnp.concatenate(away)
    return updated(meta, vectors, bases, [(away, shifted(away, "k", 1))], (2,), out)


def solution(mesh):
    torus = Mesh(mesh.devices.reshape(4, 2, 2, 2, 4), ROW + COL)
    return jax.shard_map(
        shards,
        mesh=torus,
        in_specs=(P(ROW, COL), P(COL, ROW, None), P(COL, None, None)),
        out_specs=P(ROW, COL),
        check_vma=False,
    )
```
